256 devices in a mesh: segment: 4 (over x), lane: 64 (over y, z, core).
Axes of the slice: x: 4, y: 4, z: 8, core: 2. Of those that a mesh axis runs over, the one named last changes fastest.
Arguments:
- spectra: float32 [4, 4096, 1024], P(None, 'lane'), may hold values from -6 to 6
- rfi_flags: int32 [4, 4096, 8], P(None, 'lane'), may hold values 0 or 1
- sub_delay: int32 [64, 4096], P(None, 'lane'), may hold values from 0 to 7
- fine_delay: int32 [2048, 64], P('lane'), may hold values from 0 to 31
- widths: int32 [8], replicated, may hold values from 1 to 64
Outputs:
- peaks: float32 [4, 2048, 8], P('segment', 'lane')
The draws below stay inside these ranges and needn't reach their ends.
All inputs are finite; a program needn't handle non-finite values. No bound on the sum of `rfi_flags` on one device may be relied on, other than what follows from the above.
Results may differ from the reference program's by a relative error of at most 0.0001.
Values sent between devices are 32-bit elements; how exact they have to be, the bound alone decides.
No kernel may reach another device: no remote copies, remote signals or barrier semaphores. Data moves between devices by JAX's collectives and lax.ppermute only.
A program may use at most 64 MiB of HBM per device.

```python
import jax
import jax.numpy as jnp
from jax import lax

C = 4096
SUBCH = 64
NSUB = 64
NCOARSE = 64
NDM = 2048
S = 1024
M = 4
BLK = 128
D1 = 8
D2 = 32
NW = 8
WMAX = 64


def touch_ends(array, stream_key, low, largest):
    place = [jax.random.randint(jax.random.fold_in(stream_key, axis), (), 0, length) for axis, length in enumerate(array.shape)]
    widest = array.shape.index(max(array.shape))
    neighbour = place[:widest] + [(place[widest] + 1) % array.shape[widest]] + place[widest + 1:]
    return array.at[tuple(place)].set(low).at[tuple(neighbour)].set(largest)


def levels(key, extent, shards, least, largest):
    factor_of = 1.0
    for position, parts in shards:
        draws = jax.random.uniform(jax.random.fold_in(jax.random.fold_in(key, 6), position), (parts,), jnp.float32, least / len(shards), largest / len(shards))
        factor_of = factor_of * jnp.repeat(jnp.exp(draws), extent[position] // parts).reshape((-1,) + (1,) * (len(extent) - 1 - position))
    return factor_of


def bell_draw(stream_key, extent, scale, most, split=(), kind=jnp.bfloat16):
    loudness = levels(stream_key, extent, split, -0.22, 0.18) if split else 1.0
    drawn = jax.random.normal(stream_key, extent, jnp.float32) * scale * loudness
    return jnp.minimum(jnp.maximum(drawn, -most), most).astype(kind)


def setup_inputs(seed: int = 0) -> dict:
    arg_keys = jax.random.split(jax.random.key(seed), 6)
    return {
        "spectra": bell_draw(arg_keys[0], (M, C, S), 1.0, 6.0, ((1, 64),), jnp.float32),
        "rfi_flags": touch_ends((jax.random.randint(arg_keys[1], (M, C, S // BLK), 0, 8) < 1).astype(jnp.int32), jax.random.fold_in(arg_keys[1], 1), 0, 1),
        "sub_delay": touch_ends(jax.random.randint(arg_keys[2], (NCOARSE, C), 0, D1), jax.random.fold_in(arg_keys[2], 1), 0, D1 - 1).astype(jnp.int32),
        "fine_delay": touch_ends(jax.random.randint(arg_keys[3], (NDM, NSUB), 0, D2), jax.random.fold_in(arg_keys[3], 1), 0, D2 - 1).astype(jnp.int32),
        "widths": touch_ends(jax.random.randint(arg_keys[4], (NW,), 1, WMAX + 1), jax.random.fold_in(arg_keys[4], 1), 1, WMAX).astype(jnp.int32),
    }


def clean_block(power_in, flag_rows, block_len):
    row_count, samples = power_in.shape
    kept_mask = 1.0 - flag_rows.astype(jnp.float32)
    kept_mask = jnp.broadcast_to(kept_mask[:, :, None], (row_count, flag_rows.shape[1], block_len)).reshape(row_count, samples)
    masked = kept_mask * power_in
    centre = lax.optimization_barrier(jnp.mean(masked, axis=1, keepdims=True))
    spread = lax.optimization_barrier(jnp.mean((masked - centre) * (masked - centre), axis=1, keepdims=True))
    return kept_mask * (power_in - centre) * lax.rsqrt(spread + 1e-05)

def detect(centered, widths, total_sq, cell_count):
    sigma = jnp.sqrt(total_sq / cell_count + 1e-06)
    samples = centered.shape[1]
    prefix = jnp.concatenate([jnp.zeros((centered.shape[0], 1), jnp.float32), jnp.cumsum(centered, axis=1)], axis=1)
    sample_idx = jnp.arange(samples, dtype=jnp.int32)
    ends = jnp.minimum(sample_idx[None, :] + widths[:, None], samples)
    upper = prefix[:, ends]
    lower = prefix[:, None, :samples]
    scaled = (upper - lower) / (sigma * jnp.sqrt(widths.astype(jnp.float32)))[None, :, None]
    return lax.optimization_barrier(jnp.max(scaled, axis=2))

def reference(spectra, rfi_flags, sub_delay, fine_delay, widths):
    sample_idx = jnp.arange(S, dtype=jnp.int32)
    owners = jnp.arange(NDM, dtype=jnp.int32) // (NDM // NCOARSE)
    outputs = []
    for batch in range(M):
        normed = clean_block(spectra[batch], rfi_flags[batch], BLK)
        zero_level = lax.optimization_barrier(jnp.sum(normed, axis=0)) / C
        cleaned = normed - zero_level[None, :]
        padded = jnp.pad(cleaned, ((0, 0), (0, D1)))

        def coarse_row(delay_row):
            lookup = sample_idx[None, :] + delay_row[:, None]
            picked = jnp.take_along_axis(padded, lookup, axis=1)
            return picked.reshape(NSUB, SUBCH, S).sum(axis=1)
        subbands = lax.map(coarse_row, sub_delay)
        sub_padded = jnp.pad(subbands, ((0, 0), (0, 0), (0, D2)))

        def dm_row(entry_pair):
            delay_row, owner_row = entry_pair
            source = lax.dynamic_index_in_dim(sub_padded, owner_row, 0, keepdims=False)
            lookup = sample_idx[None, :] + delay_row[:, None]
            return jnp.take_along_axis(source, lookup, axis=1).sum(axis=0)
        series = lax.map(dm_row, (fine_delay, owners))
        centered = series - lax.optimization_barrier(jnp.mean(series, axis=1, keepdims=True))
        total_sq = jnp.sum(centered * centered)
        outputs.append(detect(centered, widths, total_sq, NDM * S))
    return jnp.stack(outputs)
```

```python
import jax
import jax.numpy as jnp
from jax import lax
from jax.experimental import pallas as pl
from jax.experimental.pallas import tpu as pltpu
from jax.sharding import PartitionSpec as P

C = 4096
SUBCH = 64
NSUB = 64
NCOARSE = 64
NDM = 2048
S = 1024
D1 = 8
D2 = 32
NW = 8
JDEV = 32
LANES = 128
NCH = S // LANES
ROW = 2 * NCH + 1
SPLITS = 3
F0 = 2
F1 = D2 // F0


def lane_ids(rows):
    return lax.broadcasted_iota(jnp.int32, (rows, LANES), 1)


def shifted(chunks, amount, lane):
    if amount == 0:
        return chunks
    rolled = [pltpu.roll(c, LANES - amount, axis=1) for c in chunks]
    rolled.append(jnp.zeros_like(rolled[0]))
    return [
        jnp.where(lane < LANES - amount, rolled[c], rolled[c + 1]) for c in range(len(chunks))
    ]


def pieces(x, count):
    parts = []
    for _ in range(count):
        part = x.astype(jnp.bfloat16)
        parts.append(part)
        x = x - part.astype(jnp.float32)
    return parts


def front_kernel(seg_ref, power_ref, flags_ref, delay_ref, out_ref):
    del seg_ref
    keep = 1.0 - flags_ref[0].astype(jnp.float32)
    kept = [jnp.broadcast_to(keep[:, c : c + 1], (SUBCH, LANES)) for c in range(NCH)]
    power = [power_ref[0, :, c * LANES : (c + 1) * LANES] for c in range(NCH)]
    masked = [kept[c] * power[c] for c in range(NCH)]
    centre = jnp.sum(sum(masked), axis=1, keepdims=True) * (1.0 / S)
    spread = sum((m - centre) * (m - centre) for m in masked)
    spread = jnp.sum(spread, axis=1, keepdims=True) * (1.0 / S)
    scale = lax.rsqrt(spread + 1e-05)
    normed = [kept[c] * (power[c] - centre) * scale for c in range(NCH)]

    for c in range(NCH):
        channel_sum = jnp.sum(normed[c], axis=0, keepdims=True)
        out_ref[pl.ds(NCH + c, NCOARSE, stride=ROW), :] = jnp.broadcast_to(
            channel_sum, (NCOARSE, LANES)
        )

    delay = delay_ref[...]
    lane = lane_ids(NCOARSE)
    counts = jnp.zeros((NCOARSE, LANES), jnp.float32)
    for d in range(D1):
        count = jnp.sum((delay == d).astype(jnp.float32), axis=1, keepdims=True)
        counts = jnp.where(
            jnp.logical_and(lane % D1 == d, lane < SPLITS * D1), count, counts
        )
    out_ref[pl.ds(2 * NCH, NCOARSE, stride=ROW), :] = counts

    delay4 = jnp.concatenate([delay] * 4, axis=1)
    weights = jnp.concatenate(
        [(delay4 == d).astype(jnp.float32).astype(jnp.bfloat16) for d in range(D1)], axis=0
    )
    split = [pieces(n, SPLITS) for n in normed]
    rows = [
        jnp.concatenate([split[c][s] for c in range(NCH)], axis=1) for s in range(SPLITS)
    ]
    rows.append(jnp.zeros_like(rows[0]))
    data = jnp.concatenate(rows, axis=0)
    sums = jnp.dot(weights, data, preferred_element_type=jnp.float32)
    totals = None
    for d in range(D1):
        part = sums[d * NCOARSE : (d + 1) * NCOARSE]
        part = shifted([part[:, c * LANES : (c + 1) * LANES] for c in range(NCH)], d, lane)
        totals = part if totals is None else [a + b for a, b in zip(totals, part)]
    for c in range(NCH):
        out_ref[pl.ds(c, NCOARSE, stride=ROW), :] = totals[c]


def fine_kernel(widths_ref, moved_ref, delay_ref, square_ref, peak_ref):
    lane = lane_ids(NSUB)
    raw = [moved_ref[pl.ds(c, NSUB, stride=ROW), :] for c in range(NCH)]
    zero = [
        jnp.broadcast_to(
            jnp.sum(moved_ref[pl.ds(NCH + c, NSUB, stride=ROW), :], axis=0, keepdims=True)
            * (1.0 / C),
            (D1, LANES),
        )
        for c in range(NCH)
    ]
    counts = moved_ref[pl.ds(2 * NCH, NSUB, stride=ROW), :]

    lane8 = lane_ids(D1)
    row8 = lax.broadcasted_iota(jnp.int32, (D1, LANES), 0)
    later = zero
    for d in range(1, D1):
        moved_on = shifted(zero, d, lane8)
        later = [jnp.where(row8 == d, moved_on[c], later[c]) for c in range(NCH)]
    later = jnp.concatenate(later, axis=1)
    parts = [p.astype(jnp.float32) for p in pieces(later, SPLITS)]
    parts.append(jnp.zeros_like(parts[0]))
    zero_rows = jnp.concatenate(parts, axis=0).astype(jnp.bfloat16)
    level = jnp.dot(
        counts[:, : 4 * D1].astype(jnp.bfloat16), zero_rows, preferred_element_type=jnp.float32
    )
    subbands = [raw[c] - level[:, c * LANES : (c + 1) * LANES] for c in range(NCH)]

    delay = delay_ref[...]
    delay4 = jnp.concatenate([delay] * 4, axis=1)
    low = (lax.broadcasted_iota(jnp.int32, (JDEV, 4 * NSUB), 1) // NSUB) % F0
    weights = jnp.concatenate(
        [
            (delay4 == F0 * f + low).astype(jnp.float32).astype(jnp.bfloat16)
            for f in range(F1)
        ],
        axis=0,
    )
    by_lag = [
        pieces(jnp.concatenate(shifted(subbands, f, lane), axis=1), 2) for f in range(F0)
    ]
    data = jnp.concatenate([by_lag[f][s] for s in range(2) for f in range(F0)], axis=0)
    sums = jnp.dot(weights, data, preferred_element_type=jnp.float32)
    lane32 = lane_ids(JDEV)
    series = None
    for f in range(F1):
        part = sums[f * JDEV : (f + 1) * JDEV]
        part = shifted(
            [part[:, c * LANES : (c + 1) * LANES] for c in range(NCH)], F0 * f, lane32
        )
        series = part if series is None else [a + b for a, b in zip(series, part)]

    mean = jnp.sum(sum(series), axis=1, keepdims=True) * (1.0 / S)
    centered = [s - mean for s in series]
    square = jnp.sum(sum(x * x for x in centered))
    square_ref[...] = jnp.broadcast_to(square, square_ref.shape)

    stacked = jnp.concatenate(centered, axis=0)
    both = jnp.concatenate(pieces(stacked, 2), axis=1)
    before = lax.broadcasted_iota(jnp.int32, (2 * LANES, 2 * LANES), 0) % LANES
    column = lax.broadcasted_iota(jnp.int32, (2 * LANES, 2 * LANES), 1)
    ladder = jnp.where(
        jnp.logical_or(before < column, column >= LANES), 1.0, 0.0
    ).astype(jnp.bfloat16)
    sums = jnp.dot(both, ladder, preferred_element_type=jnp.float32)
    prefix = []
    done = jnp.zeros((JDEV, LANES), jnp.float32)
    for c in range(NCH):
        prefix.append(sums[c * JDEV : (c + 1) * JDEV, :LANES] + done)
        done = done + sums[c * JDEV : (c + 1) * JDEV, LANES:]
    peaks = jnp.zeros((JDEV, LANES), jnp.float32)
    for i in range(NW):
        width = widths_ref[i]
        rolled = [pltpu.roll(p, LANES - width, axis=1) for p in prefix] + [done]
        here = lane32 < LANES - width
        best = None
        for c in range(NCH):
            box = jnp.where(here, rolled[c], rolled[c + 1]) - prefix[c]
            best = box if best is None else jnp.maximum(best, box)
        best = jnp.max(best, axis=1, keepdims=True)
        root = lax.rsqrt(jnp.full((JDEV, LANES), width.astype(jnp.float32)))
        peaks = jnp.where(lane32 == i, best * root, peaks)
    peak_ref[...] = peaks


def last_kernel(square_ref, peak_ref, out_ref):
    total = jnp.sum(square_ref[...], axis=0, keepdims=True)
    sigma = jnp.sqrt(total * (1.0 / (NDM * S)) + 1e-06)
    out_ref[...] = (peak_ref[...] / sigma)[:, :NW]


VMEM = pl.BlockSpec(memory_space=pltpu.VMEM)
SMEM = pl.BlockSpec(memory_space=pltpu.SMEM)


def body(spectra, rfi_flags, sub_delay, fine_delay, widths):
    lanes = lax.axis_size("lane")
    seg = lax.axis_index("segment").astype(jnp.int32).reshape(1)
    message = pl.pallas_call(
        front_kernel,
        name="front",
        grid_spec=pltpu.PrefetchScalarGridSpec(
            num_scalar_prefetch=1,
            grid=(1,),
            in_specs=[
                pl.BlockSpec((1, SUBCH, S), lambda i, seg: (seg[0], 0, 0)),
                pl.BlockSpec((1, SUBCH, NCH), lambda i, seg: (seg[0], 0, 0)),
                pl.BlockSpec((NCOARSE, SUBCH), lambda i, seg: (0, 0)),
            ],
            out_specs=pl.BlockSpec((NCOARSE * ROW, LANES), lambda i, seg: (0, 0)),
        ),
        out_shape=jax.ShapeDtypeStruct((NCOARSE * ROW, LANES), jnp.float32),
    )(seg, spectra, rfi_flags, sub_delay)
    moved = lax.all_to_all(
        message.reshape(lanes, 1, ROW * LANES), "lane", split_axis=0, concat_axis=0, tiled=True
    )
    square, peaks = pl.pallas_call(
        fine_kernel,
        name="fine",
        in_specs=[SMEM, VMEM, VMEM],
        out_specs=[VMEM, VMEM],
        out_shape=[
            jax.ShapeDtypeStruct((lanes, LANES), jnp.float32),
            jax.ShapeDtypeStruct((JDEV, LANES), jnp.float32),
        ],
    )(widths, moved.reshape(lanes * ROW, LANES), fine_delay)
    squares = lax.all_to_all(
        square.reshape(lanes, 1, LANES), "lane", split_axis=0, concat_axis=0, tiled=True
    )
    out = pl.pallas_call(
        last_kernel,
        name="last",
        in_specs=[VMEM, VMEM],
        out_specs=VMEM,
        out_shape=jax.ShapeDtypeStruct((JDEV, NW), jnp.float32),
    )(squares.reshape(lanes, LANES), peaks)
    return out[None]


def solution(mesh):
    in_specs = (P(None, "lane", None), P(None, "lane", None), P(None, "lane"), P("lane", None), P())
    out_specs = P("segment", "lane", None)
    return jax.shard_map(body, mesh=mesh, in_specs=in_specs, out_specs=out_specs, check_vma=False)
```

```python
import jax
import jax.numpy as jnp
from jax import lax
from jax.experimental import pallas as pl
from jax.experimental.pallas import tpu as pltpu
from jax.sharding import PartitionSpec as P

C = 4096
SUBCH = 64
NSUB = 64
NCOARSE = 64
NDM = 2048
S = 1024
D1 = 8
D2 = 32
NW = 8
JDEV = 32
LANES = 128
NCH = S // LANES
ROW = 2 * NCH + 1
SPLITS = 3
F0 = 2
F1 = D2 // F0


def lane_ids(rows):
    return lax.broadcasted_iota(jnp.int32, (rows, LANES), 1)


def shifted(chunks, amount, lane):
    if amount == 0:
        return chunks
    rolled = [pltpu.roll(c, LANES - amount, axis=1) for c in chunks]
    rolled.append(jnp.zeros_like(rolled[0]))
    return [
        jnp.where(lane < LANES - amount, rolled[c], rolled[c + 1]) for c in range(len(chunks))
    ]


def pieces(x, count):
    parts = []
    for _ in range(count):
        part = x.astype(jnp.bfloat16)
        parts.append(part)
        x = x - part.astype(jnp.float32)
    return parts


def front_kernel(power_hbm, flags_hbm, delay_hbm, out_ref, power_ref, flags_ref, delay_ref, sems):
    mine = lax.axis_index("segment")
    copies = [
        pltpu.make_async_copy(delay_hbm, delay_ref, sems.at[0]),
        pltpu.make_async_copy(flags_hbm.at[mine], flags_ref, sems.at[1]),
        pltpu.make_async_copy(power_hbm.at[mine], power_ref, sems.at[2]),
    ]
    for copy in copies:
        copy.start()

    copies[0].wait()
    delay = delay_ref[...]
    lane = lane_ids(NCOARSE)
    counts = jnp.zeros((NCOARSE, LANES), jnp.float32)
    for d in range(D1):
        count = jnp.sum((delay == d).astype(jnp.float32), axis=1, keepdims=True)
        counts = jnp.where(
            jnp.logical_and(lane % D1 == d, lane < SPLITS * D1), count, counts
        )
    out_ref[pl.ds(2 * NCH, NCOARSE, stride=ROW), :] = counts
    delay4 = jnp.concatenate([delay] * 4, axis=1)
    weights = jnp.concatenate(
        [(delay4 == d).astype(jnp.float32).astype(jnp.bfloat16) for d in range(D1)], axis=0
    )

    copies[1].wait()
    copies[2].wait()
    keep = (1.0 - flags_ref[...].astype(jnp.float32)).astype(jnp.bfloat16)
    block = lax.broadcasted_iota(jnp.int32, (NCH, S), 1) // LANES
    own = block == lax.broadcasted_iota(jnp.int32, (NCH, S), 0)
    kept = lax.dot_general(
        keep,
        own.astype(jnp.float32).astype(jnp.bfloat16),
        (((0,), (0,)), ((), ())),
        preferred_element_type=jnp.float32,
    )
    kept = [kept[:, c * LANES : (c + 1) * LANES] for c in range(NCH)]
    power = [power_ref[:, c * LANES : (c + 1) * LANES] for c in range(NCH)]
    masked = [kept[c] * power[c] for c in range(NCH)]
    centre = jnp.sum(sum(masked), axis=1, keepdims=True) * (1.0 / S)
    spread = sum((m - centre) * (m - centre) for m in masked)
    spread = jnp.sum(spread, axis=1, keepdims=True) * (1.0 / S)
    scale = lax.rsqrt(spread + 1e-05)
    normed = [kept[c] * (power[c] - centre) * scale for c in range(NCH)]

    for c in range(NCH):
        channel_sum = jnp.sum(normed[c], axis=0, keepdims=True)
        out_ref[pl.ds(NCH + c, NCOARSE, stride=ROW), :] = jnp.broadcast_to(
            channel_sum, (NCOARSE, LANES)
        )

    split = [pieces(n, SPLITS) for n in normed]
    rows = [
        jnp.concatenate([split[c][s] for c in range(NCH)], axis=1) for s in range(SPLITS)
    ]
    rows.append(jnp.zeros_like(rows[0]))
    data = jnp.concatenate(rows, axis=0)
    sums = jnp.dot(weights, data, preferred_element_type=jnp.float32)
    totals = None
    for d in range(D1):
        part = sums[d * NCOARSE : (d + 1) * NCOARSE]
        part = shifted([part[:, c * LANES : (c + 1) * LANES] for c in range(NCH)], d, lane)
        totals = part if totals is None else [a + b for a, b in zip(totals, part)]
    for c in range(NCH):
        out_ref[pl.ds(c, NCOARSE, stride=ROW), :] = totals[c]


def fine_kernel(widths_hbm, moved_ref, delay_ref, square_ref, peak_ref, widths_ref, sem):
    fetch = pltpu.make_async_copy(widths_hbm, widths_ref, sem)
    fetch.start()
    lane = lane_ids(NSUB)
    raw = [moved_ref[pl.ds(c, NSUB, stride=ROW), :] for c in range(NCH)]
    zero = [
        jnp.broadcast_to(
            jnp.sum(moved_ref[pl.ds(NCH + c, NSUB, stride=ROW), :], axis=0, keepdims=True)
            * (1.0 / C),
            (D1, LANES),
        )
        for c in range(NCH)
    ]
    counts = moved_ref[pl.ds(2 * NCH, NSUB, stride=ROW), :]

    lane8 = lane_ids(D1)
    row8 = lax.broadcasted_iota(jnp.int32, (D1, LANES), 0)
    later = zero
    for d in range(1, D1):
        moved_on = shifted(zero, d, lane8)
        later = [jnp.where(row8 == d, moved_on[c], later[c]) for c in range(NCH)]
    later = jnp.concatenate(later, axis=1)
    parts = [p.astype(jnp.float32) for p in pieces(later, SPLITS)]
    parts.append(jnp.zeros_like(parts[0]))
    zero_rows = jnp.concatenate(parts, axis=0).astype(jnp.bfloat16)
    level = jnp.dot(
        counts[:, : 4 * D1].astype(jnp.bfloat16), zero_rows, preferred_element_type=jnp.float32
    )
    subbands = [raw[c] - level[:, c * LANES : (c + 1) * LANES] for c in range(NCH)]

    delay = delay_ref[...]
    delay4 = jnp.concatenate([delay] * 4, axis=1)
    low = (lax.broadcasted_iota(jnp.int32, (JDEV, 4 * NSUB), 1) // NSUB) % F0
    weights = jnp.concatenate(
        [
            (delay4 == F0 * f + low).astype(jnp.float32).astype(jnp.bfloat16)
            for f in range(F1)
        ],
        axis=0,
    )
    by_lag = [
        pieces(jnp.concatenate(shifted(subbands, f, lane), axis=1), 2) for f in range(F0)
    ]
    data = jnp.concatenate([by_lag[f][s] for s in range(2) for f in range(F0)], axis=0)
    sums = jnp.dot(weights, data, preferred_element_type=jnp.float32)
    lane32 = lane_ids(JDEV)
    series = None
    for f in range(F1):
        part = sums[f * JDEV : (f + 1) * JDEV]
        part = shifted(
            [part[:, c * LANES : (c + 1) * LANES] for c in range(NCH)], F0 * f, lane32
        )
        series = part if series is None else [a + b for a, b in zip(series, part)]

    mean = jnp.sum(sum(series), axis=1, keepdims=True) * (1.0 / S)
    centered = [s - mean for s in series]
    square = jnp.sum(sum(x * x for x in centered))
    square_ref[...] = jnp.broadcast_to(square, square_ref.shape)

    stacked = jnp.concatenate(centered, axis=0)
    both = jnp.concatenate(pieces(stacked, 2), axis=1)
    before = lax.broadcasted_iota(jnp.int32, (2 * LANES, 2 * LANES), 0) % LANES
    column = lax.broadcasted_iota(jnp.int32, (2 * LANES, 2 * LANES), 1)
    ladder = jnp.where(
        jnp.logical_or(before < column, column >= LANES), 1.0, 0.0
    ).astype(jnp.bfloat16)
    sums = jnp.dot(both, ladder, preferred_element_type=jnp.float32)
    prefix = []
    done = jnp.zeros((JDEV, LANES), jnp.float32)
    for c in range(NCH):
        prefix.append(sums[c * JDEV : (c + 1) * JDEV, :LANES] + done)
        done = done + sums[c * JDEV : (c + 1) * JDEV, LANES:]
    peaks = jnp.zeros((JDEV, LANES), jnp.float32)
    fetch.wait()
    for i in range(NW):
        width = widths_ref[i]
        rolled = [pltpu.roll(p, LANES - width, axis=1) for p in prefix] + [done]
        here = lane32 < LANES - width
        best = None
        for c in range(NCH):
            box = jnp.where(here, rolled[c], rolled[c + 1]) - prefix[c]
            best = box if best is None else jnp.maximum(best, box)
        best = jnp.max(best, axis=1, keepdims=True)
        root = lax.rsqrt(jnp.full((JDEV, LANES), width.astype(jnp.float32)))
        peaks = jnp.where(lane32 == i, best * root, peaks)
    peak_ref[...] = peaks.T[:NW]


def last_kernel(square_ref, peak_ref, out_ref):
    total = jnp.sum(square_ref[...], axis=0, keepdims=True)
    sigma = jnp.sqrt(total * (1.0 / (NDM * S)) + 1e-06)
    out_ref[...] = peak_ref[...] / sigma[:, :JDEV]


VMEM = pl.BlockSpec(memory_space=pltpu.VMEM)
ANY = pl.BlockSpec(memory_space=pl.ANY)
PARAMS = pltpu.CompilerParams(vmem_limit_bytes=32 * 1024 * 1024)


def in_hbm(x):
    return pltpu.with_memory_space_constraint(x, pltpu.HBM)


def in_vmem(x):
    return pltpu.with_memory_space_constraint(x, pltpu.VMEM)


def body(spectra, rfi_flags, sub_delay, fine_delay, widths):
    lanes = lax.axis_size("lane")
    message = pl.pallas_call(
        front_kernel,
        name="front",
        in_specs=[ANY, ANY, ANY],
        out_specs=VMEM,
        out_shape=pltpu.VMEM((NCOARSE * ROW, LANES), jnp.float32),
        scratch_shapes=[
            pltpu.VMEM((SUBCH, S), jnp.float32),
            pltpu.VMEM((NCH, SUBCH), jnp.int32),
            pltpu.VMEM((NCOARSE, SUBCH), jnp.int32),
            pltpu.SemaphoreType.DMA((3,)),
        ],
        compiler_params=PARAMS,
    )(in_hbm(spectra), in_hbm(jnp.transpose(rfi_flags, (0, 2, 1))), in_hbm(sub_delay))
    moved = lax.all_to_all(
        message.reshape(lanes, 1, ROW * LANES), "lane", split_axis=0, concat_axis=0, tiled=True
    )
    square, peaks = pl.pallas_call(
        fine_kernel,
        name="fine",
        in_specs=[ANY, VMEM, VMEM],
        out_specs=[VMEM, VMEM],
        out_shape=[
            pltpu.VMEM((lanes, LANES), jnp.float32),
            pltpu.VMEM((NW, JDEV), jnp.float32),
        ],
        scratch_shapes=[pltpu.SMEM((NW,), jnp.int32), pltpu.SemaphoreType.DMA],
        compiler_params=PARAMS,
    )(in_hbm(widths), in_vmem(moved.reshape(lanes * ROW, LANES)), fine_delay)
    squares = lax.all_to_all(
        square.reshape(lanes, 1, LANES), "lane", split_axis=0, concat_axis=0, tiled=True
    )
    out = pl.pallas_call(
        last_kernel,
        name="last",
        in_specs=[VMEM, VMEM],
        out_specs=VMEM,
        out_shape=jax.ShapeDtypeStruct((NW, JDEV), jnp.float32),
        compiler_params=PARAMS,
    )(in_vmem(squares.reshape(lanes, LANES)), peaks)
    return out.T[None]


def solution(mesh):
    in_specs = (P(None, "lane", None), P(None, "lane", None), P(None, "lane"), P("lane", None), P())
    out_specs = P("segment", "lane", None)
    return jax.shard_map(body, mesh=mesh, in_specs=in_specs, out_specs=out_specs, check_vma=False)
```

```python
import jax
import jax.numpy as jnp
from jax import lax
from jax.experimental import pallas as pl
from jax.experimental.pallas import tpu as pltpu
from jax.sharding import PartitionSpec as P

C = 4096
SUBCH = 64
NSUB = 64
NCOARSE = 64
NDM = 2048
S = 1024
D1 = 8
D2 = 32
NW = 8
WMAX = 64
GAP = 2
JDEV = 32
LANES = 128
NCH = S // LANES
ROW = 2 * NCH + 1
SPLITS = 3
FINE_SPLITS = 2
ORDER = (37, 11, 21)


def peer(i):
    i = (i * ORDER[0] + ORDER[1]) & 63
    i = i ^ (i >> 3)
    i = (i * ORDER[2]) & 63
    return i ^ (i >> 2)


def lane_ids(rows):
    return lax.broadcasted_iota(jnp.int32, (rows, LANES), 1)


def shifted(chunks, amount, lane):
    if amount == 0:
        return chunks
    rolled = [pltpu.roll(c, LANES - amount, axis=1) for c in chunks]
    rolled.append(jnp.zeros_like(rolled[0]))
    return [
        jnp.where(lane < LANES - amount, rolled[c], rolled[c + 1]) for c in range(len(chunks))
    ]


def pieces(x, count):
    parts = []
    for _ in range(count):
        part = x.astype(jnp.bfloat16)
        parts.append(part)
        x = x - part.astype(jnp.float32)
    return parts


def lag_rows(chunks, lags, count, lane):
    by_lag = [pieces(jnp.concatenate(shifted(chunks, f, lane), axis=1), count) for f in range(lags)]
    return jnp.concatenate([by_lag[f][s] for s in range(count) for f in range(lags)], axis=0)


def selector(shape, axis):
    place = lax.broadcasted_iota(jnp.int32, shape, axis) % 64
    lane = lax.broadcasted_iota(jnp.int32, shape, 1 - axis)
    return (lane == peer(place)).astype(jnp.float32).astype(jnp.bfloat16)


def small(delay):
    return delay.astype(jnp.float32).astype(jnp.bfloat16)


def one_hot(wide, width, groups):
    lag = (lax.broadcasted_iota(jnp.int32, wide.shape, 1) // width) % 2
    wide = wide - lag.astype(jnp.float32)
    return jnp.concatenate(
        [(wide == 2.0 * g).astype(jnp.float32).astype(jnp.bfloat16) for g in range(groups)],
        axis=0,
    )


def front_kernel(
    power_hbm, flags_hbm, delay_hbm, widths_hbm, out_ref, widths_ref, power_ref, flags_ref, delay_ref, sems
):
    mine = lax.axis_index("segment")
    widths_copy = pltpu.make_async_copy(widths_hbm, widths_ref, sems.at[3])
    copies = [
        pltpu.make_async_copy(delay_hbm, delay_ref, sems.at[0]),
        pltpu.make_async_copy(flags_hbm.at[mine], flags_ref, sems.at[1]),
        pltpu.make_async_copy(power_hbm.at[mine], power_ref, sems.at[2]),
    ]
    for copy in copies:
        copy.start()
    widths_copy.start()

    copies[0].wait()
    delay = jnp.dot(
        selector((NCOARSE, NCOARSE), 0),
        small(delay_ref[...]),
        preferred_element_type=jnp.float32,
    )
    lane = lane_ids(NCOARSE)
    counts = jnp.zeros((NCOARSE, LANES), jnp.float32)
    for d in range(D1):
        count = jnp.sum((delay == float(d)).astype(jnp.float32), axis=1, keepdims=True)
        counts = jnp.where(
            jnp.logical_and(lane % D1 == d, lane < SPLITS * D1), count, counts
        )
    out_ref[pl.ds(2 * NCH, NCOARSE, stride=ROW), :] = counts
    weights = one_hot(jnp.concatenate([delay] * (2 * SPLITS), axis=1), SUBCH, D1 // 2)

    copies[1].wait()
    keep = (1.0 - flags_ref[...].astype(jnp.float32)).astype(jnp.bfloat16)
    block = lax.broadcasted_iota(jnp.int32, (NCH, S), 1) // LANES
    own = block == lax.broadcasted_iota(jnp.int32, (NCH, S), 0)
    kept = lax.dot_general(
        keep,
        own.astype(jnp.float32).astype(jnp.bfloat16),
        (((0,), (0,)), ((), ())),
        preferred_element_type=jnp.float32,
    )
    kept = [kept[:, c * LANES : (c + 1) * LANES] for c in range(NCH)]
    copies[2].wait()
    power = [power_ref[:, c * LANES : (c + 1) * LANES] for c in range(NCH)]
    masked = [kept[c] * power[c] for c in range(NCH)]
    centre = jnp.sum(sum(masked), axis=1, keepdims=True) * (1.0 / S)
    spread = sum((m - centre) * (m - centre) for m in masked)
    spread = jnp.sum(spread, axis=1, keepdims=True) * (1.0 / S)
    scale = lax.rsqrt(spread + 1e-05)
    normed = [kept[c] * (power[c] - centre) * scale for c in range(NCH)]

    for c in range(NCH):
        channel_sum = jnp.sum(normed[c], axis=0, keepdims=True)
        out_ref[pl.ds(NCH + c, NCOARSE, stride=ROW), :] = jnp.broadcast_to(
            channel_sum, (NCOARSE, LANES)
        )

    data = lag_rows(normed, 2, SPLITS, lane)
    sums = jnp.dot(weights, data, preferred_element_type=jnp.float32)
    totals = None
    for d in range(D1 // 2):
        part = sums[d * NCOARSE : (d + 1) * NCOARSE]
        part = shifted([part[:, c * LANES : (c + 1) * LANES] for c in range(NCH)], 2 * d, lane)
        totals = part if totals is None else [a + b for a, b in zip(totals, part)]
    for c in range(NCH):
        out_ref[pl.ds(c, NCOARSE, stride=ROW), :] = totals[c]
    widths_copy.wait()


def fine_kernel(widths_ref, moved_ref, delay_ref, square_ref, peak_ref, ramp_ref):
    lane = lane_ids(NSUB)
    raw = [moved_ref[pl.ds(c, NSUB, stride=ROW), :] for c in range(NCH)]
    zero = [
        jnp.broadcast_to(
            jnp.sum(moved_ref[pl.ds(NCH + c, NSUB, stride=ROW), :], axis=0, keepdims=True)
            * (1.0 / C),
            (D1, LANES),
        )
        for c in range(NCH)
    ]
    counts = moved_ref[pl.ds(2 * NCH, NSUB, stride=ROW), :]

    lane8 = lane_ids(D1)
    row8 = lax.broadcasted_iota(jnp.int32, (D1, LANES), 0)
    later = zero
    for d in range(1, D1):
        moved_on = shifted(zero, d, lane8)
        later = [jnp.where(row8 == d, moved_on[c], later[c]) for c in range(NCH)]
    later = jnp.concatenate(later, axis=1)
    parts = [p.astype(jnp.float32) for p in pieces(later, SPLITS)]
    parts.append(jnp.zeros_like(parts[0]))
    zero_rows = jnp.concatenate(parts, axis=0).astype(jnp.bfloat16)
    level = jnp.dot(
        counts[:, : 4 * D1].astype(jnp.bfloat16), zero_rows, preferred_element_type=jnp.float32
    )
    subbands = [raw[c] - level[:, c * LANES : (c + 1) * LANES] for c in range(NCH)]

    wide = jnp.dot(
        small(delay_ref[...]),
        selector((NSUB, 2 * FINE_SPLITS * NSUB), 1),
        preferred_element_type=jnp.float32,
    )
    weights = one_hot(wide, NSUB, D2 // 2)
    data = lag_rows(subbands, 2, FINE_SPLITS, lane)
    sums = jnp.dot(weights, data, preferred_element_type=jnp.float32)
    lane32 = lane_ids(JDEV)
    series = None
    for f in range(D2 // 2):
        part = sums[f * JDEV : (f + 1) * JDEV]
        part = shifted(
            [part[:, c * LANES : (c + 1) * LANES] for c in range(NCH)], 2 * f, lane32
        )
        series = part if series is None else [a + b for a, b in zip(series, part)]

    mean = jnp.sum(sum(series), axis=1, keepdims=True) * (1.0 / S)
    centered = [s - mean for s in series]
    square = jnp.sum(sum(x * x for x in centered))
    square_ref[...] = jnp.broadcast_to(square, square_ref.shape)

    half = NCH // 2
    across = jnp.concatenate(
        [jnp.concatenate(centered[h * half : (h + 1) * half], axis=0).T for h in range(2)], axis=1
    )
    data = jnp.concatenate(pieces(across, FINE_SPLITS), axis=0)
    shape = (LANES + 8, FINE_SPLITS * LANES)
    ladder = lax.broadcasted_iota(jnp.int32, shape, 1) % LANES < lax.broadcasted_iota(
        jnp.int32, shape, 0
    )
    ramp = jnp.dot(
        ladder.astype(jnp.float32).astype(jnp.bfloat16), data, preferred_element_type=jnp.float32
    )
    lane = lane_ids(WMAX)
    total = jnp.broadcast_to(ramp[LANES : LANES + 1], (WMAX, 2 * LANES))
    first = pltpu.roll(ramp[:WMAX, :LANES], LANES - JDEV, axis=1)
    second = pltpu.roll(ramp[:WMAX, LANES:], LANES - JDEV, axis=1)
    follow = lane < LANES - JDEV
    low = [ramp[:LANES, :LANES], ramp[:LANES, LANES:]]
    high = [
        total[:, :LANES] + jnp.where(follow, first, second),
        total[:, LANES:] + jnp.where(follow, second, 0.0),
    ]
    for h in range(2):
        ramp_ref[h, pl.ds(0, LANES, stride=GAP), :] = low[h]
        ramp_ref[h, pl.ds(GAP * LANES, WMAX, stride=GAP), :] = high[h]
    row8 = lax.broadcasted_iota(jnp.int32, (NW, 2 * LANES), 0)
    peaks = jnp.zeros((NW, 2 * LANES), jnp.float32)
    for i in range(NW):
        width = widths_ref[i]
        best = [
            jnp.max(ramp_ref[h, pl.ds(GAP * width, LANES, stride=GAP), :] - low[h], axis=0, keepdims=True)
            for h in range(2)
        ]
        best = jnp.concatenate(best, axis=1)
        root = lax.rsqrt(jnp.full((1, 2 * LANES), width.astype(jnp.float32)))
        peaks = jnp.where(row8 == i, best * root, peaks)
    best = jnp.maximum(peaks[:, :LANES], peaks[:, LANES:])
    best = jnp.maximum(best, pltpu.roll(best, 2 * JDEV, axis=1))
    best = jnp.maximum(best, pltpu.roll(best, JDEV, axis=1))
    peak_ref[...] = best[:, :JDEV]


def last_kernel(square_ref, peak_ref, out_ref):
    total = jnp.sum(square_ref[...], axis=0, keepdims=True)
    sigma = jnp.sqrt(total * (1.0 / (NDM * S)) + 1e-06)
    out_ref[...] = peak_ref[...] / sigma[:, :JDEV]


GROUP = [[peer(i) for i in range(NCOARSE)]]
VMEM = pl.BlockSpec(memory_space=pltpu.VMEM)
SMEM = pl.BlockSpec(memory_space=pltpu.SMEM)
ANY = pl.BlockSpec(memory_space=pl.ANY)
PARAMS = pltpu.CompilerParams(vmem_limit_bytes=32 * 1024 * 1024)


def in_hbm(x):
    return pltpu.with_memory_space_constraint(x, pltpu.HBM)


def in_vmem(x):
    return pltpu.with_memory_space_constraint(x, pltpu.VMEM)


def body(spectra, rfi_flags, sub_delay, fine_delay, widths):
    lanes = lax.axis_size("lane")
    message, widths = pl.pallas_call(
        front_kernel,
        name="front",
        in_specs=[ANY, ANY, ANY, ANY],
        out_specs=[VMEM, SMEM],
        out_shape=[
            pltpu.VMEM((NCOARSE * ROW, LANES), jnp.float32),
            pltpu.SMEM((NW,), jnp.int32),
        ],
        scratch_shapes=[
            pltpu.VMEM((SUBCH, S), jnp.float32),
            pltpu.VMEM((NCH, SUBCH), jnp.int32),
            pltpu.VMEM((NCOARSE, SUBCH), jnp.int32),
            pltpu.SemaphoreType.DMA((4,)),
        ],
        compiler_params=PARAMS,
    )(in_hbm(spectra), in_hbm(jnp.transpose(rfi_flags, (0, 2, 1))), in_hbm(sub_delay), in_hbm(widths))
    moved = lax.all_to_all(
        message.reshape(lanes, 1, ROW * LANES), "lane", split_axis=0, concat_axis=0, tiled=True, axis_index_groups=GROUP
    )
    square, peaks = pl.pallas_call(
        fine_kernel,
        name="fine",
        in_specs=[SMEM, VMEM, VMEM],
        out_specs=[VMEM, VMEM],
        out_shape=[
            pltpu.VMEM((lanes, LANES), jnp.float32),
            pltpu.VMEM((NW, JDEV), jnp.float32),
        ],
        scratch_shapes=[pltpu.VMEM((2, GAP * (LANES + WMAX), LANES), jnp.float32)],
        compiler_params=PARAMS,
    )(pltpu.with_memory_space_constraint(widths, pltpu.SMEM), in_vmem(moved.reshape(lanes * ROW, LANES)), fine_delay)
    squares = lax.all_to_all(
        square.reshape(lanes, 1, LANES), "lane", split_axis=0, concat_axis=0, tiled=True, axis_index_groups=GROUP
    )
    out = pl.pallas_call(
        last_kernel,
        name="last",
        in_specs=[VMEM, VMEM],
        out_specs=VMEM,
        out_shape=jax.ShapeDtypeStruct((NW, JDEV), jnp.float32),
        compiler_params=PARAMS,
    )(in_vmem(squares.reshape(lanes, LANES)), peaks)
    return out.T[None]


def solution(mesh):
    in_specs = (P(None, "lane", None), P(None, "lane", None), P(None, "lane"), P("lane", None), P())
    out_specs = P("segment", "lane", None)
    return jax.shard_map(body, mesh=mesh, in_specs=in_specs, out_specs=out_specs, check_vma=False)
```

```python
import jax
import jax.numpy as jnp
from jax import lax
from jax.experimental import pallas as pl
from jax.experimental.pallas import tpu as pltpu
from jax.sharding import PartitionSpec as P

C = 4096
SUBCH = 64
NSUB = 64
NCOARSE = 64
NDM = 2048
S = 1024
D1 = 8
D2 = 32
NW = 8
WMAX = 64
GAP = 2
JDEV = 32
LANES = 128
NCH = S // LANES
ROW = 2 * NCH + 1
SPLITS = 3
FINE_SPLITS = 2
LAGS1 = 4
LAGS2 = 4
ORDER = (57, 59, 57)


def peer(i):
    i = (i * ORDER[0] + ORDER[1]) & 63
    i = i ^ (i >> 3)
    i = (i * ORDER[2]) & 63
    return i ^ (i >> 2)


def lane_ids(rows):
    return lax.broadcasted_iota(jnp.int32, (rows, LANES), 1)


def shifted(chunks, amount, lane):
    if amount == 0:
        return chunks
    rolled = [pltpu.roll(c, LANES - amount, axis=1) for c in chunks]
    rolled.append(jnp.zeros_like(rolled[0]))
    return [
        jnp.where(lane < LANES - amount, rolled[c], rolled[c + 1]) for c in range(len(chunks))
    ]


def pieces(x, count):
    parts = []
    for _ in range(count):
        part = x.astype(jnp.bfloat16)
        parts.append(part)
        x = x - part.astype(jnp.float32)
    return parts


def lag_rows(chunks, lags, count, lane):
    by_lag = [pieces(jnp.concatenate(shifted(chunks, f, lane), axis=1), count) for f in range(lags)]
    return jnp.concatenate([by_lag[f][s] for s in range(count) for f in range(lags)], axis=0)


def selector(shape, axis):
    place = lax.broadcasted_iota(jnp.int32, shape, axis) % 64
    lane = lax.broadcasted_iota(jnp.int32, shape, 1 - axis)
    return (lane == peer(place)).astype(jnp.float32).astype(jnp.bfloat16)


def small(delay):
    return delay.astype(jnp.float32).astype(jnp.bfloat16)


def one_hot(wide, width, lags, groups):
    lag = (lax.broadcasted_iota(jnp.int32, wide.shape, 1) // width) % lags
    wide = wide - lag.astype(jnp.float32)
    return jnp.concatenate(
        [
            (wide == float(lags * g)).astype(jnp.float32).astype(jnp.bfloat16)
            for g in range(groups)
        ],
        axis=0,
    )


def front_kernel(
    power_hbm, flags_hbm, delay_hbm, widths_hbm, out_ref, widths_ref, power_ref, flags_ref, delay_ref, sems
):
    mine = lax.axis_index("segment")
    widths_copy = pltpu.make_async_copy(widths_hbm, widths_ref, sems.at[3])
    copies = [
        pltpu.make_async_copy(delay_hbm, delay_ref, sems.at[0]),
        pltpu.make_async_copy(flags_hbm.at[mine], flags_ref, sems.at[1]),
        pltpu.make_async_copy(power_hbm.at[mine], power_ref, sems.at[2]),
    ]
    for copy in copies:
        copy.start()
    widths_copy.start()

    copies[0].wait()
    delay = jnp.dot(
        selector((NCOARSE, NCOARSE), 0),
        small(delay_ref[...]),
        preferred_element_type=jnp.float32,
    )
    lane = lane_ids(NCOARSE)
    counts = jnp.zeros((NCOARSE, LANES), jnp.float32)
    for d in range(D1):
        count = jnp.sum((delay == float(d)).astype(jnp.float32), axis=1, keepdims=True)
        counts = jnp.where(
            jnp.logical_and(lane % D1 == D1 - 1 - d, lane < SPLITS * D1), count, counts
        )
    out_ref[pl.ds(2 * NCH, NCOARSE, stride=ROW), :] = counts
    weights = one_hot(jnp.concatenate([delay] * (LAGS1 * SPLITS), axis=1), SUBCH, LAGS1, D1 // LAGS1)

    copies[1].wait()
    keep = (1.0 - flags_ref[...].astype(jnp.float32)).astype(jnp.bfloat16)
    block = lax.broadcasted_iota(jnp.int32, (NCH, S), 1) // LANES
    own = block == lax.broadcasted_iota(jnp.int32, (NCH, S), 0)
    kept = lax.dot_general(
        keep,
        own.astype(jnp.float32).astype(jnp.bfloat16),
        (((0,), (0,)), ((), ())),
        preferred_element_type=jnp.float32,
    )
    kept = [kept[:, c * LANES : (c + 1) * LANES] for c in range(NCH)]
    copies[2].wait()
    power = [power_ref[:, c * LANES : (c + 1) * LANES] for c in range(NCH)]
    masked = [kept[c] * power[c] for c in range(NCH)]
    centre = jnp.sum(sum(masked), axis=1, keepdims=True) * (1.0 / S)
    spread = sum((m - centre) * (m - centre) for m in masked)
    spread = jnp.sum(spread, axis=1, keepdims=True) * (1.0 / S)
    scale = lax.rsqrt(spread + 1e-05)
    normed = [kept[c] * (power[c] - centre) * scale for c in range(NCH)]

    for c in range(NCH):
        channel_sum = jnp.sum(normed[c], axis=0, keepdims=True)
        out_ref[pl.ds(NCH + c, NCOARSE, stride=ROW), :] = jnp.broadcast_to(
            channel_sum, (NCOARSE, LANES)
        )

    data = lag_rows(normed, LAGS1, SPLITS, lane)
    sums = jnp.dot(weights, data, preferred_element_type=jnp.float32)
    totals = None
    for d in range(D1 // LAGS1):
        part = sums[d * NCOARSE : (d + 1) * NCOARSE]
        part = shifted([part[:, c * LANES : (c + 1) * LANES] for c in range(NCH)], LAGS1 * d, lane)
        totals = part if totals is None else [a + b for a, b in zip(totals, part)]
    for c in range(NCH):
        out_ref[pl.ds(c, NCOARSE, stride=ROW), :] = totals[c]
    widths_copy.wait()


def fine_kernel(widths_ref, moved_ref, delay_ref, square_ref, peak_ref, ramp_ref):
    lane = lane_ids(NSUB)
    raw = [moved_ref[pl.ds(c, NSUB, stride=ROW), :] for c in range(NCH)]
    zero = [
        jnp.broadcast_to(
            jnp.sum(moved_ref[pl.ds(NCH + c, NSUB, stride=ROW), :], axis=0, keepdims=True)
            * (1.0 / C),
            (D1, LANES),
        )
        for c in range(NCH)
    ]
    counts = moved_ref[pl.ds(2 * NCH, NSUB, stride=ROW), :]

    row = lax.broadcasted_iota(jnp.int32, (D1, LANES), 0)
    rolled = [
        pltpu.roll(z, LANES - (D1 - 1), axis=1, stride=1, stride_axis=0) for z in zero
    ] + [jnp.zeros((D1, LANES), jnp.float32)]
    later = [
        jnp.where(lane_ids(D1) < LANES - (D1 - 1) + row, rolled[c], rolled[c + 1])
        for c in range(NCH)
    ]
    later = jnp.concatenate(later, axis=1)
    parts = [p.astype(jnp.float32) for p in pieces(later, SPLITS)]
    parts.append(jnp.zeros_like(parts[0]))
    zero_rows = jnp.concatenate(parts, axis=0).astype(jnp.bfloat16)
    level = jnp.dot(
        counts[:, : 4 * D1].astype(jnp.bfloat16), zero_rows, preferred_element_type=jnp.float32
    )
    subbands = [raw[c] - level[:, c * LANES : (c + 1) * LANES] for c in range(NCH)]

    wide = jnp.dot(
        small(delay_ref[...]),
        selector((NSUB, LAGS2 * FINE_SPLITS * NSUB), 1),
        preferred_element_type=jnp.float32,
    )
    weights = one_hot(wide, NSUB, LAGS2, D2 // LAGS2)
    data = lag_rows(subbands, LAGS2, FINE_SPLITS, lane)
    sums = jnp.dot(weights, data, preferred_element_type=jnp.float32)
    lane32 = lane_ids(JDEV)
    series = None
    for f in range(D2 // LAGS2):
        part = sums[f * JDEV : (f + 1) * JDEV]
        part = shifted(
            [part[:, c * LANES : (c + 1) * LANES] for c in range(NCH)], LAGS2 * f, lane32
        )
        series = part if series is None else [a + b for a, b in zip(series, part)]

    mean = jnp.sum(sum(series), axis=1, keepdims=True) * (1.0 / S)
    centered = [s - mean for s in series]
    square = jnp.sum(sum(x * x for x in centered))
    square_ref[...] = jnp.broadcast_to(square, square_ref.shape)

    half = NCH // 2
    across = jnp.concatenate(
        [jnp.concatenate(centered[h * half : (h + 1) * half], axis=0).T for h in range(2)], axis=1
    )
    data = jnp.concatenate(pieces(across, FINE_SPLITS), axis=0)
    shape = (LANES + 8, FINE_SPLITS * LANES)
    ladder = lax.broadcasted_iota(jnp.int32, shape, 1) % LANES < lax.broadcasted_iota(
        jnp.int32, shape, 0
    )
    ramp = jnp.dot(
        ladder.astype(jnp.float32).astype(jnp.bfloat16), data, preferred_element_type=jnp.float32
    )
    lane = lane_ids(WMAX)
    total = jnp.broadcast_to(ramp[LANES : LANES + 1], (WMAX, 2 * LANES))
    first = pltpu.roll(ramp[:WMAX, :LANES], LANES - JDEV, axis=1)
    second = pltpu.roll(ramp[:WMAX, LANES:], LANES - JDEV, axis=1)
    follow = lane < LANES - JDEV
    low = [ramp[:LANES, :LANES], ramp[:LANES, LANES:]]
    high = [
        total[:, :LANES] + jnp.where(follow, first, second),
        total[:, LANES:] + jnp.where(follow, second, 0.0),
    ]
    for h in range(2):
        ramp_ref[h, pl.ds(0, LANES, stride=GAP), :] = low[h]
        ramp_ref[h, pl.ds(GAP * LANES, WMAX, stride=GAP), :] = high[h]
    row8 = lax.broadcasted_iota(jnp.int32, (NW, 2 * LANES), 0)
    peaks = jnp.zeros((NW, 2 * LANES), jnp.float32)
    for i in range(NW):
        width = widths_ref[i]
        best = [
            jnp.max(ramp_ref[h, pl.ds(GAP * width, LANES, stride=GAP), :] - low[h], axis=0, keepdims=True)
            for h in range(2)
        ]
        best = jnp.concatenate(best, axis=1)
        root = lax.rsqrt(jnp.full((1, 2 * LANES), width.astype(jnp.float32)))
        peaks = jnp.where(row8 == i, best * root, peaks)
    best = jnp.maximum(peaks[:, :LANES], peaks[:, LANES:])
    best = jnp.maximum(best, pltpu.roll(best, 2 * JDEV, axis=1))
    best = jnp.maximum(best, pltpu.roll(best, JDEV, axis=1))
    peak_ref[...] = best[:, :JDEV]


def last_kernel(square_ref, peak_ref, out_ref):
    total = jnp.sum(square_ref[...], axis=0, keepdims=True)
    sigma = jnp.sqrt(total * (1.0 / (NDM * S)) + 1e-06)
    out_ref[...] = peak_ref[...] / sigma[:, :JDEV]


NOISE_ORDER = [39, 20, 55, 48, 17, 0, 16, 50, 1, 33, 35, 9, 31, 49, 54, 36, 15, 11, 59, 3, 29, 19, 10, 30, 27, 34, 24, 44, 63, 7, 28, 12, 46, 47, 61, 45, 32, 21, 62, 25, 22, 60, 4, 56, 40, 52, 38, 37, 23, 18, 41, 6, 2, 51, 43, 8, 57, 26, 13, 58, 5, 14, 42, 53]
GROUP = [[peer(i) for i in range(NCOARSE)]]
VMEM = pl.BlockSpec(memory_space=pltpu.VMEM)
SMEM = pl.BlockSpec(memory_space=pltpu.SMEM)
ANY = pl.BlockSpec(memory_space=pl.ANY)
PARAMS = pltpu.CompilerParams(vmem_limit_bytes=32 * 1024 * 1024)


def in_hbm(x):
    return pltpu.with_memory_space_constraint(x, pltpu.HBM)


def in_vmem(x):
    return pltpu.with_memory_space_constraint(x, pltpu.VMEM)


def body(spectra, rfi_flags, sub_delay, fine_delay, widths):
    lanes = lax.axis_size("lane")
    message, widths = pl.pallas_call(
        front_kernel,
        name="front",
        in_specs=[ANY, ANY, ANY, ANY],
        out_specs=[VMEM, SMEM],
        out_shape=[
            pltpu.VMEM((NCOARSE * ROW, LANES), jnp.float32),
            pltpu.SMEM((NW,), jnp.int32),
        ],
        scratch_shapes=[
            pltpu.VMEM((SUBCH, S), jnp.float32),
            pltpu.VMEM((NCH, SUBCH), jnp.int32),
            pltpu.VMEM((NCOARSE, SUBCH), jnp.int32),
            pltpu.SemaphoreType.DMA((4,)),
        ],
        compiler_params=PARAMS,
    )(in_hbm(spectra), in_hbm(jnp.transpose(rfi_flags, (0, 2, 1))), in_hbm(sub_delay), in_hbm(widths))
    moved = lax.all_to_all(
        message.reshape(lanes, 1, ROW * LANES), "lane", split_axis=0, concat_axis=0, tiled=True, axis_index_groups=GROUP
    )
    square, peaks = pl.pallas_call(
        fine_kernel,
        name="fine",
        in_specs=[SMEM, VMEM, VMEM],
        out_specs=[VMEM, VMEM],
        out_shape=[
            pltpu.VMEM((lanes, LANES), jnp.float32),
            pltpu.VMEM((NW, JDEV), jnp.float32),
        ],
        scratch_shapes=[pltpu.VMEM((2, GAP * (LANES + WMAX), LANES), jnp.float32)],
        compiler_params=PARAMS,
    )(pltpu.with_memory_space_constraint(widths, pltpu.SMEM), in_vmem(moved.reshape(lanes * ROW, LANES)), fine_delay)
    squares = lax.all_to_all(
        square.reshape(lanes, 1, LANES), "lane", split_axis=0, concat_axis=0, tiled=True, axis_index_groups=[NOISE_ORDER]
    )
    out = pl.pallas_call(
        last_kernel,
        name="last",
        in_specs=[VMEM, VMEM],
        out_specs=VMEM,
        out_shape=jax.ShapeDtypeStruct((NW, JDEV), jnp.float32),
        compiler_params=PARAMS,
    )(in_vmem(squares.reshape(lanes, LANES)), peaks)
    return out.T[None]


def solution(mesh):
    in_specs = (P(None, "lane", None), P(None, "lane", None), P(None, "lane"), P("lane", None), P())
    out_specs = P("segment", "lane", None)
    return jax.shard_map(body, mesh=mesh, in_specs=in_specs, out_specs=out_specs, check_vma=False)
```

```python
import jax
import jax.numpy as jnp
from jax import lax
from jax.experimental import pallas as pl
from jax.experimental.pallas import tpu as pltpu
from jax.sharding import PartitionSpec as P

C = 4096
SUBCH = 64
NSUB = 64
NCOARSE = 64
NDM = 2048
S = 1024
D1 = 8
D2 = 32
NW = 8
WMAX = 64
GAP = 2
JDEV = 32
LANES = 128
NCH = S // LANES
ROW = 2 * NCH + 1
SPLITS = 3
FINE_SPLITS = 2
LAGS1 = 4
LAGS2 = 4
ORDER = (51, 17, 49)


def peer(i):
    i = (i * ORDER[0] + ORDER[1]) & 63
    i = i ^ (i >> 3)
    i = (i * ORDER[2]) & 63
    return i ^ (i >> 2)


def lane_ids(rows):
    return lax.broadcasted_iota(jnp.int32, (rows, LANES), 1)


def shifted(chunks, amount, lane):
    if amount == 0:
        return chunks
    rolled = [pltpu.roll(c, LANES - amount, axis=1) for c in chunks]
    rolled.append(jnp.zeros_like(rolled[0]))
    return [
        jnp.where(lane < LANES - amount, rolled[c], rolled[c + 1]) for c in range(len(chunks))
    ]


def pieces(x, count):
    parts = []
    for _ in range(count):
        part = x.astype(jnp.bfloat16)
        parts.append(part)
        x = x - part.astype(jnp.float32)
    return parts


def lag_rows(chunks, lags, count, lane):
    by_lag = [pieces(jnp.concatenate(shifted(chunks, f, lane), axis=1), count) for f in range(lags)]
    return jnp.concatenate([by_lag[f][s] for s in range(count) for f in range(lags)], axis=0)


def selector(shape, axis):
    place = lax.broadcasted_iota(jnp.int32, shape, axis) % 64
    lane = lax.broadcasted_iota(jnp.int32, shape, 1 - axis)
    return (lane == peer(place)).astype(jnp.float32).astype(jnp.bfloat16)


def small(delay):
    return delay.astype(jnp.float32).astype(jnp.bfloat16)


def one_hot(wide, width, lags, groups):
    lag = (lax.broadcasted_iota(jnp.int32, wide.shape, 1) // width) % lags
    wide = wide - lag.astype(jnp.float32)
    return jnp.concatenate(
        [
            (wide == float(lags * g)).astype(jnp.float32).astype(jnp.bfloat16)
            for g in range(groups)
        ],
        axis=0,
    )


def front_kernel(
    power_hbm, flags_hbm, delay_hbm, widths_hbm, out_ref, widths_ref, power_ref, flags_ref, delay_ref, sems
):
    mine = lax.axis_index("segment")
    widths_copy = pltpu.make_async_copy(widths_hbm, widths_ref, sems.at[3])
    copies = [
        pltpu.make_async_copy(delay_hbm, delay_ref, sems.at[0]),
        pltpu.make_async_copy(flags_hbm.at[mine], flags_ref, sems.at[1]),
        pltpu.make_async_copy(power_hbm.at[mine], power_ref, sems.at[2]),
    ]
    for copy in copies:
        copy.start()
    widths_copy.start()

    copies[0].wait()
    delay = jnp.dot(
        selector((NCOARSE, NCOARSE), 0),
        small(delay_ref[...]),
        preferred_element_type=jnp.float32,
    )
    lane = lane_ids(NCOARSE)
    counts = jnp.zeros((NCOARSE, LANES), jnp.float32)
    for d in range(D1):
        count = jnp.sum((delay == float(d)).astype(jnp.float32), axis=1, keepdims=True)
        counts = jnp.where(
            jnp.logical_and(lane % D1 == D1 - 1 - d, lane < SPLITS * D1), count, counts
        )
    out_ref[pl.ds(2 * NCH, NCOARSE, stride=ROW), :] = counts
    weights = one_hot(jnp.concatenate([delay] * (LAGS1 * SPLITS), axis=1), SUBCH, LAGS1, D1 // LAGS1)

    copies[1].wait()
    keep = (1.0 - flags_ref[...].astype(jnp.float32)).astype(jnp.bfloat16)
    block = lax.broadcasted_iota(jnp.int32, (NCH, S), 1) // LANES
    own = block == lax.broadcasted_iota(jnp.int32, (NCH, S), 0)
    kept = lax.dot_general(
        keep,
        own.astype(jnp.float32).astype(jnp.bfloat16),
        (((0,), (0,)), ((), ())),
        preferred_element_type=jnp.float32,
    )
    kept = [kept[:, c * LANES : (c + 1) * LANES] for c in range(NCH)]
    copies[2].wait()
    power = [power_ref[:, c * LANES : (c + 1) * LANES] for c in range(NCH)]
    masked = [kept[c] * power[c] for c in range(NCH)]
    centre = jnp.sum(sum(masked), axis=1, keepdims=True) * (1.0 / S)
    spread = sum((m - centre) * (m - centre) for m in masked)
    spread = jnp.sum(spread, axis=1, keepdims=True) * (1.0 / S)
    scale = lax.rsqrt(spread + 1e-05)
    normed = [kept[c] * (power[c] - centre) * scale for c in range(NCH)]

    for c in range(NCH):
        channel_sum = jnp.sum(normed[c], axis=0, keepdims=True)
        out_ref[pl.ds(NCH + c, NCOARSE, stride=ROW), :] = jnp.broadcast_to(
            channel_sum, (NCOARSE, LANES)
        )

    data = lag_rows(normed, LAGS1, SPLITS, lane)
    sums = jnp.dot(weights, data, preferred_element_type=jnp.float32)
    totals = None
    for d in range(D1 // LAGS1):
        part = sums[d * NCOARSE : (d + 1) * NCOARSE]
        part = shifted([part[:, c * LANES : (c + 1) * LANES] for c in range(NCH)], LAGS1 * d, lane)
        totals = part if totals is None else [a + b for a, b in zip(totals, part)]
    for c in range(NCH):
        out_ref[pl.ds(c, NCOARSE, stride=ROW), :] = totals[c]
    widths_copy.wait()


def fine_kernel(widths_ref, moved_ref, delay_ref, square_ref, peak_ref, ramp_ref):
    lane = lane_ids(NSUB)
    raw = [moved_ref[pl.ds(c, NSUB, stride=ROW), :] for c in range(NCH)]
    zero = [
        jnp.broadcast_to(
            jnp.sum(moved_ref[pl.ds(NCH + c, NSUB, stride=ROW), :], axis=0, keepdims=True)
            * (1.0 / C),
            (D1, LANES),
        )
        for c in range(NCH)
    ]
    counts = moved_ref[pl.ds(2 * NCH, NSUB, stride=ROW), :]

    row = lax.broadcasted_iota(jnp.int32, (D1, LANES), 0)
    rolled = [
        pltpu.roll(z, LANES - (D1 - 1), axis=1, stride=1, stride_axis=0) for z in zero
    ] + [jnp.zeros((D1, LANES), jnp.float32)]
    later = [
        jnp.where(lane_ids(D1) < LANES - (D1 - 1) + row, rolled[c], rolled[c + 1])
        for c in range(NCH)
    ]
    later = jnp.concatenate(later, axis=1)
    parts = [p.astype(jnp.float32) for p in pieces(later, SPLITS)]
    parts.append(jnp.zeros_like(parts[0]))
    zero_rows = jnp.concatenate(parts, axis=0).astype(jnp.bfloat16)
    level = jnp.dot(
        counts[:, : 4 * D1].astype(jnp.bfloat16), zero_rows, preferred_element_type=jnp.float32
    )
    subbands = [raw[c] - level[:, c * LANES : (c + 1) * LANES] for c in range(NCH)]

    wide = jnp.dot(
        small(delay_ref[...]),
        selector((NSUB, LAGS2 * FINE_SPLITS * NSUB), 1),
        preferred_element_type=jnp.float32,
    )
    weights = one_hot(wide, NSUB, LAGS2, D2 // LAGS2)
    data = lag_rows(subbands, LAGS2, FINE_SPLITS, lane)
    sums = jnp.dot(weights, data, preferred_element_type=jnp.float32)
    lane32 = lane_ids(JDEV)
    series = None
    for f in range(D2 // LAGS2):
        part = sums[f * JDEV : (f + 1) * JDEV]
        part = shifted(
            [part[:, c * LANES : (c + 1) * LANES] for c in range(NCH)], LAGS2 * f, lane32
        )
        series = part if series is None else [a + b for a, b in zip(series, part)]

    mean = jnp.sum(sum(series), axis=1, keepdims=True) * (1.0 / S)
    centered = [s - mean for s in series]
    square = jnp.sum(sum(x * x for x in centered))
    square_ref[...] = jnp.broadcast_to(square, square_ref.shape)

    half = NCH // 2
    across = jnp.concatenate(
        [jnp.concatenate(centered[h * half : (h + 1) * half], axis=0).T for h in range(2)], axis=1
    )
    data = jnp.concatenate(pieces(across, FINE_SPLITS), axis=0)
    shape = (LANES + 8, FINE_SPLITS * LANES)
    ladder = lax.broadcasted_iota(jnp.int32, shape, 1) % LANES < lax.broadcasted_iota(
        jnp.int32, shape, 0
    )
    ramp = jnp.dot(
        ladder.astype(jnp.float32).astype(jnp.bfloat16), data, preferred_element_type=jnp.float32
    )
    lane = lane_ids(WMAX)
    total = jnp.broadcast_to(ramp[LANES : LANES + 1], (WMAX, 2 * LANES))
    first = pltpu.roll(ramp[:WMAX, :LANES], LANES - JDEV, axis=1)
    second = pltpu.roll(ramp[:WMAX, LANES:], LANES - JDEV, axis=1)
    follow = lane < LANES - JDEV
    low = [ramp[:LANES, :LANES], ramp[:LANES, LANES:]]
    high = [
        total[:, :LANES] + jnp.where(follow, first, second),
        total[:, LANES:] + jnp.where(follow, second, 0.0),
    ]
    for h in range(2):
        ramp_ref[h, pl.ds(0, LANES, stride=GAP), :] = low[h]
        ramp_ref[h, pl.ds(GAP * LANES, WMAX, stride=GAP), :] = high[h]
    row8 = lax.broadcasted_iota(jnp.int32, (NW, 2 * LANES), 0)
    peaks = jnp.zeros((NW, 2 * LANES), jnp.float32)
    for i in range(NW):
        width = widths_ref[i]
        best = [
            jnp.max(ramp_ref[h, pl.ds(GAP * width, LANES, stride=GAP), :] - low[h], axis=0, keepdims=True)
            for h in range(2)
        ]
        best = jnp.concatenate(best, axis=1)
        root = lax.rsqrt(jnp.full((1, 2 * LANES), width.astype(jnp.float32)))
        peaks = jnp.where(row8 == i, best * root, peaks)
    best = jnp.maximum(peaks[:, :LANES], peaks[:, LANES:])
    best = jnp.maximum(best, pltpu.roll(best, 2 * JDEV, axis=1))
    best = jnp.maximum(best, pltpu.roll(best, JDEV, axis=1))
    peak_ref[...] = best[:, :JDEV]


def last_kernel(square_ref, peak_ref, out_ref):
    total = jnp.sum(square_ref[...], axis=0, keepdims=True)
    sigma = jnp.sqrt(total * (1.0 / (NDM * S)) + 1e-06)
    out_ref[...] = peak_ref[...] / sigma[:, :JDEV]


NOISE_ORDER = [
    57, 32, 24, 20, 31, 61, 17, 1, 53, 5, 10, 43, 44, 59, 0, 36,
    4, 35, 38, 33, 14, 50, 51, 60, 18, 7, 11, 55, 22, 63, 39, 19,
    30, 3, 54, 2, 27, 29, 58, 13, 45, 37, 34, 56, 16, 41, 25, 52,
    49, 47, 62, 46, 23, 6, 15, 9, 28, 26, 40, 8, 42, 12, 48, 21,
]
GROUP = [[peer(i) for i in range(NCOARSE)]]
VMEM = pl.BlockSpec(memory_space=pltpu.VMEM)
SMEM = pl.BlockSpec(memory_space=pltpu.SMEM)
ANY = pl.BlockSpec(memory_space=pl.ANY)
PARAMS = pltpu.CompilerParams(vmem_limit_bytes=32 * 1024 * 1024)


def in_hbm(x):
    return pltpu.with_memory_space_constraint(x, pltpu.HBM)


def in_vmem(x):
    return pltpu.with_memory_space_constraint(x, pltpu.VMEM)


def body(spectra, rfi_flags, sub_delay, fine_delay, widths):
    lanes = lax.axis_size("lane")
    message, widths = pl.pallas_call(
        front_kernel,
        name="front",
        in_specs=[ANY, ANY, ANY, ANY],
        out_specs=[VMEM, SMEM],
        out_shape=[
            pltpu.VMEM((NCOARSE * ROW, LANES), jnp.float32),
            pltpu.SMEM((NW,), jnp.int32),
        ],
        scratch_shapes=[
            pltpu.VMEM((SUBCH, S), jnp.float32),
            pltpu.VMEM((NCH, SUBCH), jnp.int32),
            pltpu.VMEM((NCOARSE, SUBCH), jnp.int32),
            pltpu.SemaphoreType.DMA((4,)),
        ],
        compiler_params=PARAMS,
    )(in_hbm(spectra), in_hbm(jnp.transpose(rfi_flags, (0, 2, 1))), in_hbm(sub_delay), in_hbm(widths))
    moved = lax.all_to_all(
        message.reshape(lanes, 1, ROW * LANES), "lane", split_axis=0, concat_axis=0, tiled=True, axis_index_groups=GROUP
    )
    square, peaks = pl.pallas_call(
        fine_kernel,
        name="fine",
        in_specs=[SMEM, VMEM, VMEM],
        out_specs=[VMEM, VMEM],
        out_shape=[
            pltpu.VMEM((lanes, LANES), jnp.float32),
            pltpu.VMEM((NW, JDEV), jnp.float32),
        ],
        scratch_shapes=[pltpu.VMEM((2, GAP * (LANES + WMAX), LANES), jnp.float32)],
        compiler_params=PARAMS,
    )(pltpu.with_memory_space_constraint(widths, pltpu.SMEM), in_vmem(moved.reshape(lanes * ROW, LANES)), fine_delay)
    squares = lax.all_to_all(
        square.reshape(lanes, 1, LANES), "lane", split_axis=0, concat_axis=0, tiled=True, axis_index_groups=[NOISE_ORDER]
    )
    out = pl.pallas_call(
        last_kernel,
        name="last",
        in_specs=[VMEM, VMEM],
        out_specs=VMEM,
        out_shape=jax.ShapeDtypeStruct((NW, JDEV), jnp.float32),
        compiler_params=PARAMS,
    )(in_vmem(squares.reshape(lanes, LANES)), peaks)
    return out.T[None]


def solution(mesh):
    in_specs = (P(None, "lane", None), P(None, "lane", None), P(None, "lane"), P("lane", None), P())
    out_specs = P("segment", "lane", None)
    return jax.shard_map(body, mesh=mesh, in_specs=in_specs, out_specs=out_specs, check_vma=False)
```

```python
import jax
import jax.numpy as jnp
from jax import lax
from jax.experimental import pallas as pl
from jax.experimental.pallas import tpu as pltpu
from jax.sharding import PartitionSpec as P

C = 4096
SUBCH = 64
NSUB = 64
NCOARSE = 64
NDM = 2048
S = 1024
D1 = 8
D2 = 32
NW = 8
WMAX = 64
GAP = 2
JDEV = 32
LANES = 128
NCH = S // LANES
ROW = 2 * NCH + 1
SPLITS = 3
FINE_SPLITS = 2
LAGS1 = 4
LAGS2 = 4
ORDER = (49, 44, 43)


def peer(i):
    i = (i * ORDER[0] + ORDER[1]) & 63
    i = i ^ (i >> 3)
    i = (i * ORDER[2]) & 63
    return i ^ (i >> 2)


def lane_ids(rows):
    return lax.broadcasted_iota(jnp.int32, (rows, LANES), 1)


def shifted(chunks, amount, lane):
    if amount == 0:
        return chunks
    rolled = [pltpu.roll(c, LANES - amount, axis=1) for c in chunks]
    rolled.append(jnp.zeros_like(rolled[0]))
    return [
        jnp.where(lane < LANES - amount, rolled[c], rolled[c + 1]) for c in range(len(chunks))
    ]


def pieces(x, count):
    parts = []
    for _ in range(count):
        part = x.astype(jnp.bfloat16)
        parts.append(part)
        x = x - part.astype(jnp.float32)
    return parts


def lag_rows(chunks, lags, count, lane):
    by_lag = [pieces(jnp.concatenate(shifted(chunks, f, lane), axis=1), count) for f in range(lags)]
    return jnp.concatenate([by_lag[f][s] for s in range(count) for f in range(lags)], axis=0)


def selector(shape, axis):
    place = lax.broadcasted_iota(jnp.int32, shape, axis) % 64
    lane = lax.broadcasted_iota(jnp.int32, shape, 1 - axis)
    return (lane == peer(place)).astype(jnp.float32).astype(jnp.bfloat16)


def small(delay):
    return delay.astype(jnp.float32).astype(jnp.bfloat16)


def one_hot(wide, width, lags, groups):
    lag = (lax.broadcasted_iota(jnp.int32, wide.shape, 1) // width) % lags
    wide = wide - lag.astype(jnp.float32)
    return jnp.concatenate(
        [
            (wide == float(lags * g)).astype(jnp.float32).astype(jnp.bfloat16)
            for g in range(groups)
        ],
        axis=0,
    )


def front_kernel(
    power_hbm, flags_hbm, delay_hbm, widths_hbm, out_ref, widths_ref, power_ref, flags_ref, delay_ref, sems
):
    mine = lax.axis_index("segment")
    widths_copy = pltpu.make_async_copy(widths_hbm, widths_ref, sems.at[3])
    copies = [
        pltpu.make_async_copy(delay_hbm, delay_ref, sems.at[0]),
        pltpu.make_async_copy(flags_hbm.at[mine], flags_ref, sems.at[1]),
        pltpu.make_async_copy(power_hbm.at[mine], power_ref, sems.at[2]),
    ]
    for copy in copies:
        copy.start()
    widths_copy.start()

    copies[0].wait()
    delay = jnp.dot(
        selector((NCOARSE, NCOARSE), 0),
        small(delay_ref[...]),
        preferred_element_type=jnp.float32,
    )
    lane = lane_ids(NCOARSE)
    counts = jnp.zeros((NCOARSE, LANES), jnp.float32)
    for d in range(D1):
        count = jnp.sum((delay == float(d)).astype(jnp.float32), axis=1, keepdims=True)
        counts = jnp.where(
            jnp.logical_and(lane % D1 == D1 - 1 - d, lane < SPLITS * D1), count, counts
        )
    out_ref[pl.ds(2 * NCH, NCOARSE, stride=ROW), :] = counts
    weights = one_hot(jnp.concatenate([delay] * (LAGS1 * SPLITS), axis=1), SUBCH, LAGS1, D1 // LAGS1)

    copies[1].wait()
    keep = (1.0 - flags_ref[...].astype(jnp.float32)).astype(jnp.bfloat16)
    block = lax.broadcasted_iota(jnp.int32, (NCH, S), 1) // LANES
    own = block == lax.broadcasted_iota(jnp.int32, (NCH, S), 0)
    kept = lax.dot_general(
        keep,
        own.astype(jnp.float32).astype(jnp.bfloat16),
        (((0,), (0,)), ((), ())),
        preferred_element_type=jnp.float32,
    )
    kept = [kept[:, c * LANES : (c + 1) * LANES] for c in range(NCH)]
    copies[2].wait()
    power = [power_ref[:, c * LANES : (c + 1) * LANES] for c in range(NCH)]
    masked = [kept[c] * power[c] for c in range(NCH)]
    centre = jnp.sum(sum(masked), axis=1, keepdims=True) * (1.0 / S)
    spread = sum((m - centre) * (m - centre) for m in masked)
    spread = jnp.sum(spread, axis=1, keepdims=True) * (1.0 / S)
    scale = lax.rsqrt(spread + 1e-05)
    normed = [kept[c] * (power[c] - centre) * scale for c in range(NCH)]

    for c in range(NCH):
        channel_sum = jnp.sum(normed[c], axis=0, keepdims=True)
        out_ref[pl.ds(NCH + c, NCOARSE, stride=ROW), :] = jnp.broadcast_to(
            channel_sum, (NCOARSE, LANES)
        )

    data = lag_rows(normed, LAGS1, SPLITS, lane)
    sums = jnp.dot(weights, data, preferred_element_type=jnp.float32)
    totals = None
    for d in range(D1 // LAGS1):
        part = sums[d * NCOARSE : (d + 1) * NCOARSE]
        part = shifted([part[:, c * LANES : (c + 1) * LANES] for c in range(NCH)], LAGS1 * d, lane)
        totals = part if totals is None else [a + b for a, b in zip(totals, part)]
    for c in range(NCH):
        out_ref[pl.ds(c, NCOARSE, stride=ROW), :] = totals[c]
    widths_copy.wait()


def fine_kernel(widths_ref, moved_ref, delay_ref, square_ref, peak_ref, ramp_ref):
    lane = lane_ids(NSUB)
    raw = [moved_ref[pl.ds(c, NSUB, stride=ROW), :] for c in range(NCH)]
    zero = [
        jnp.broadcast_to(
            jnp.sum(moved_ref[pl.ds(NCH + c, NSUB, stride=ROW), :], axis=0, keepdims=True)
            * (1.0 / C),
            (D1, LANES),
        )
        for c in range(NCH)
    ]
    counts = moved_ref[pl.ds(2 * NCH, NSUB, stride=ROW), :]

    row = lax.broadcasted_iota(jnp.int32, (D1, LANES), 0)
    rolled = [
        pltpu.roll(z, LANES - (D1 - 1), axis=1, stride=1, stride_axis=0) for z in zero
    ] + [jnp.zeros((D1, LANES), jnp.float32)]
    later = [
        jnp.where(lane_ids(D1) < LANES - (D1 - 1) + row, rolled[c], rolled[c + 1])
        for c in range(NCH)
    ]
    later = jnp.concatenate(later, axis=1)
    parts = [p.astype(jnp.float32) for p in pieces(later, SPLITS)]
    parts.append(jnp.zeros_like(parts[0]))
    zero_rows = jnp.concatenate(parts, axis=0).astype(jnp.bfloat16)
    level = jnp.dot(
        counts[:, : 4 * D1].astype(jnp.bfloat16), zero_rows, preferred_element_type=jnp.float32
    )
    subbands = [raw[c] - level[:, c * LANES : (c + 1) * LANES] for c in range(NCH)]

    wide = jnp.dot(
        small(delay_ref[...]),
        selector((NSUB, LAGS2 * FINE_SPLITS * NSUB), 1),
        preferred_element_type=jnp.float32,
    )
    weights = one_hot(wide, NSUB, LAGS2, D2 // LAGS2)
    data = lag_rows(subbands, LAGS2, FINE_SPLITS, lane)
    sums = jnp.dot(weights, data, preferred_element_type=jnp.float32)
    lane32 = lane_ids(JDEV)
    series = None
    for f in range(D2 // LAGS2):
        part = sums[f * JDEV : (f + 1) * JDEV]
        part = shifted(
            [part[:, c * LANES : (c + 1) * LANES] for c in range(NCH)], LAGS2 * f, lane32
        )
        series = part if series is None else [a + b for a, b in zip(series, part)]

    mean = jnp.sum(sum(series), axis=1, keepdims=True) * (1.0 / S)
    centered = [s - mean for s in series]
    square = jnp.sum(sum(x * x for x in centered))
    square_ref[...] = jnp.broadcast_to(square, square_ref.shape)

    half = NCH // 2
    across = jnp.concatenate(
        [jnp.concatenate(centered[h * half : (h + 1) * half], axis=0).T for h in range(2)], axis=1
    )
    data = jnp.concatenate(pieces(across, FINE_SPLITS), axis=0)
    shape = (LANES + 8, FINE_SPLITS * LANES)
    ladder = lax.broadcasted_iota(jnp.int32, shape, 1) % LANES < lax.broadcasted_iota(
        jnp.int32, shape, 0
    )
    ramp = jnp.dot(
        ladder.astype(jnp.float32).astype(jnp.bfloat16), data, preferred_element_type=jnp.float32
    )
    lane = lane_ids(WMAX)
    total = jnp.broadcast_to(ramp[LANES : LANES + 1], (WMAX, 2 * LANES))
    first = pltpu.roll(ramp[:WMAX, :LANES], LANES - JDEV, axis=1)
    second = pltpu.roll(ramp[:WMAX, LANES:], LANES - JDEV, axis=1)
    follow = lane < LANES - JDEV
    low = [ramp[:LANES, :LANES], ramp[:LANES, LANES:]]
    high = [
        total[:, :LANES] + jnp.where(follow, first, second),
        total[:, LANES:] + jnp.where(follow, second, 0.0),
    ]
    for h in range(2):
        ramp_ref[h, pl.ds(0, LANES, stride=GAP), :] = low[h]
        ramp_ref[h, pl.ds(GAP * LANES, WMAX, stride=GAP), :] = high[h]
    row8 = lax.broadcasted_iota(jnp.int32, (NW, 2 * LANES), 0)
    peaks = jnp.zeros((NW, 2 * LANES), jnp.float32)
    for i in range(NW):
        width = widths_ref[i]
        best = [
            jnp.max(ramp_ref[h, pl.ds(GAP * width, LANES, stride=GAP), :] - low[h], axis=0, keepdims=True)
            for h in range(2)
        ]
        best = jnp.concatenate(best, axis=1)
        root = lax.rsqrt(jnp.full((1, 2 * LANES), width.astype(jnp.float32)))
        peaks = jnp.where(row8 == i, best * root, peaks)
    best = jnp.maximum(peaks[:, :LANES], peaks[:, LANES:])
    best = jnp.maximum(best, pltpu.roll(best, 2 * JDEV, axis=1))
    best = jnp.maximum(best, pltpu.roll(best, JDEV, axis=1))
    peak_ref[...] = best[:, :JDEV]


def last_kernel(square_ref, peak_ref, out_ref):
    total = jnp.sum(square_ref[...], axis=0, keepdims=True)
    sigma = jnp.sqrt(total * (1.0 / (NDM * S)) + 1e-06)
    out_ref[...] = peak_ref[...] / sigma[:, :JDEV]


NOISE_ORDER = [
    57, 32, 24, 20, 31, 61, 17, 1, 53, 5, 10, 43, 44, 59, 0, 36,
    4, 35, 38, 33, 14, 50, 51, 60, 18, 7, 11, 55, 22, 63, 39, 19,
    30, 3, 54, 2, 27, 29, 58, 13, 45, 37, 34, 56, 16, 41, 25, 52,
    49, 47, 62, 46, 23, 6, 15, 9, 28, 26, 40, 8, 42, 12, 48, 21,
]
GROUP = [[peer(i) for i in range(NCOARSE)]]
VMEM = pl.BlockSpec(memory_space=pltpu.VMEM)
SMEM = pl.BlockSpec(memory_space=pltpu.SMEM)
ANY = pl.BlockSpec(memory_space=pl.ANY)
PARAMS = pltpu.CompilerParams(vmem_limit_bytes=32 * 1024 * 1024)


def in_hbm(x):
    return pltpu.with_memory_space_constraint(x, pltpu.HBM)


def in_vmem(x):
    return pltpu.with_memory_space_constraint(x, pltpu.VMEM)


def body(spectra, rfi_flags, sub_delay, fine_delay, widths):
    lanes = lax.axis_size("lane")
    message, widths = pl.pallas_call(
        front_kernel,
        name="front",
        in_specs=[ANY, ANY, ANY, ANY],
        out_specs=[VMEM, SMEM],
        out_shape=[
            pltpu.VMEM((NCOARSE * ROW, LANES), jnp.float32),
            pltpu.SMEM((NW,), jnp.int32),
        ],
        scratch_shapes=[
            pltpu.VMEM((SUBCH, S), jnp.float32),
            pltpu.VMEM((NCH, SUBCH), jnp.int32),
            pltpu.VMEM((NCOARSE, SUBCH), jnp.int32),
            pltpu.SemaphoreType.DMA((4,)),
        ],
        compiler_params=PARAMS,
    )(in_hbm(spectra), in_hbm(jnp.transpose(rfi_flags, (0, 2, 1))), in_hbm(sub_delay), in_hbm(widths))
    moved = lax.all_to_all(
        message.reshape(lanes, 1, ROW * LANES), "lane", split_axis=0, concat_axis=0, tiled=True, axis_index_groups=GROUP
    )
    square, peaks = pl.pallas_call(
        fine_kernel,
        name="fine",
        in_specs=[SMEM, VMEM, VMEM],
        out_specs=[VMEM, VMEM],
        out_shape=[
            pltpu.VMEM((lanes, LANES), jnp.float32),
            pltpu.VMEM((NW, JDEV), jnp.float32),
        ],
        scratch_shapes=[pltpu.VMEM((2, GAP * (LANES + WMAX), LANES), jnp.float32)],
        compiler_params=PARAMS,
    )(pltpu.with_memory_space_constraint(widths, pltpu.SMEM), in_vmem(moved.reshape(lanes * ROW, LANES)), fine_delay)
    squares = lax.all_to_all(
        square.reshape(lanes, 1, LANES), "lane", split_axis=0, concat_axis=0, tiled=True, axis_index_groups=[NOISE_ORDER]
    )
    out = pl.pallas_call(
        last_kernel,
        name="last",
        in_specs=[VMEM, VMEM],
        out_specs=VMEM,
        out_shape=jax.ShapeDtypeStruct((NW, JDEV), jnp.float32),
        compiler_params=PARAMS,
    )(in_vmem(squares.reshape(lanes, LANES)), peaks)
    return out.T[None]


def solution(mesh):
    in_specs = (P(None, "lane", None), P(None, "lane", None), P(None, "lane"), P("lane", None), P())
    out_specs = P("segment", "lane", None)
    return jax.shard_map(body, mesh=mesh, in_specs=in_specs, out_specs=out_specs, check_vma=False)
```
